32 devices in a mesh: rep: 2 (over x), dp: 16 (over y, z, core).
Axes of the slice: x: 2, y: 2, z: 4, core: 2. Of those that a mesh axis runs over, the one named last changes fastest.
Arguments:
- g_w_gate: bfloat16 [32, 2, 1280, 4096], P(('rep', 'dp')), parts along dimension 0
- g_w_up: bfloat16 [32, 2, 1280, 4096], P(('rep', 'dp')), parts along dimension 0
- g_w_down: bfloat16 [32, 2, 4096, 1280], P(('rep', 'dp')), parts along dimension 0
- w_gate: bfloat16 [2, 1280, 4096], replicated
- w_up: bfloat16 [2, 1280, 4096], replicated
- w_down: bfloat16 [2, 4096, 1280], replicated
- m_w_gate: float32 [2, 1280, 4096], P(None, 'dp')
- m_w_up: float32 [2, 1280, 4096], P(None, 'dp')
- m_w_down: float32 [2, 4096, 1280], P(None, 'dp')
- v_w_gate: float32 [2, 1280, 4096], P(None, 'dp')
- v_w_up: float32 [2, 1280, 4096], P(None, 'dp')
- v_w_down: float32 [2, 4096, 1280], P(None, 'dp')
Outputs:
- output 1: bfloat16 [4, 1280, 4096], P('rep'), parts along dimension 0
- output 2: bfloat16 [4, 1280, 4096], P('rep'), parts along dimension 0
- output 3: bfloat16 [4, 4096, 1280], P('rep'), parts along dimension 0
- output 4: float32 [4, 1280, 4096], P('rep', 'dp'), parts along dimension 0
- output 5: float32 [4, 1280, 4096], P('rep', 'dp'), parts along dimension 0
- output 6: float32 [4, 4096, 1280], P('rep', 'dp'), parts along dimension 0
- output 7: float32 [4, 1280, 4096], P('rep', 'dp'), parts along dimension 0
- output 8: float32 [4, 1280, 4096], P('rep', 'dp'), parts along dimension 0
- output 9: float32 [4, 4096, 1280], P('rep', 'dp'), parts along dimension 0
There are 2 independent parts. The reference program is written for one: setup_inputs(seed, part) draws one part's arguments, and reference() takes and returns one part's arrays. A program takes and returns all parts, laid end to end along the dimension named above; an argument that names none is the same for every part.
All inputs are finite; a program needn't handle non-finite values.
Results may differ from the reference program's by a relative error of at most 0.022.
Values are sent between devices in bfloat16 or wider.
A program may use at most 2 GiB of HBM per device.

```python
import jax
import jax.numpy as jnp
from jax import lax

DEVICES = 16
D = 1280
FF = 4096
LAYERS = 2
NAMES = ("w_gate", "w_up", "w_down")
SHAPES = {"w_gate": (LAYERS, D, FF), "w_up": (LAYERS, D, FF), "w_down": (LAYERS, FF, D)}


def setup_inputs(seed: int = 0, part: int = 0) -> dict:
    kz, *keys = jax.random.split(jax.random.key(seed), 1 + 5 * len(NAMES))
    loud = 2.0 ** jax.random.uniform(kz, (), jnp.float32, -1.0, 1.0)
    drawn = {}
    for name, key, both in zip(NAMES, keys[:3], keys[3:6], strict=True):
        own = jax.random.normal(jax.random.fold_in(key, part), (DEVICES, *SHAPES[name]), jnp.float32)
        shared = jax.random.normal(jax.random.fold_in(both, part), SHAPES[name], jnp.float32)
        drawn["g_" + name] = (loud * (0.7 * shared / DEVICES + 0.7 * own * DEVICES**-0.5)).astype(jnp.bfloat16)
    for name, key in zip(NAMES, keys[6:9], strict=True):
        drawn[name] = (jax.random.normal(key, SHAPES[name], jnp.float32) * SHAPES[name][1] ** -0.5).astype(jnp.bfloat16)
    for name, key in zip(NAMES, keys[9:12], strict=True):
        drawn["m_" + name] = loud * 0.5 * jax.random.normal(key, SHAPES[name], jnp.float32)
    for name, key in zip(NAMES, keys[12:15], strict=True):
        drawn["v_" + name] = loud * loud * jax.random.uniform(key, SHAPES[name], jnp.float32, 0.5, 1.5)
    return drawn


def adamw(w, m, v, g):
    m = 0.9 * m + 0.1 * g
    v = 0.95 * v + 0.05 * g * g
    step = m * lax.rsqrt(v + 1e-8) + 0.1 * w
    return (w - 0.02 * step).astype(jnp.bfloat16), m, v


def reference(g_w_gate, g_w_up, g_w_down, w_gate, w_up, w_down, m_w_gate, m_w_up, m_w_down, v_w_gate, v_w_up, v_w_down):
    def total(terms):
        return lax.scan(lambda so_far, term: (so_far + term.astype(jnp.float32), None), jnp.zeros(terms.shape[1:], jnp.float32), terms)[0]

    gradients = [total(terms).astype(jnp.bfloat16).astype(jnp.float32) for terms in (g_w_gate, g_w_up, g_w_down)]
    new = [
        adamw(w.astype(jnp.float32), m, v, g)
        for w, m, v, g in zip((w_gate, w_up, w_down), (m_w_gate, m_w_up, m_w_down), (v_w_gate, v_w_up, v_w_down), gradients, strict=True)
    ]
    return tuple(one[which] for which in range(3) for one in new)
```

```python
import functools

import jax
import jax.numpy as jnp
from jax import lax
from jax.experimental import pallas as pl
from jax.experimental.pallas import tpu as pltpu
from jax.sharding import PartitionSpec as P

MESH = pl.DeviceIdType.MESH
F32, BF16 = jnp.float32, jnp.bfloat16
Y, Z, C = 2, 4, 2
SPLIT = 16
RING = 8
SENDS = 4
DRAIN = 2
LAST = 10 + DRAIN


def kernel(split, tiles, *refs):
    g, w, m, v = (refs[i : i + 3] for i in (0, 3, 6, 9))
    out, moments = refs[12:14]
    (own_a, part_a, y_a, l_a, r_a, sy_a, sl_a, sr_a, own_b, part_b, y_b, l_b, r_b, sy_b, sl_b, sr_b) = refs[14:30]
    (w_a, m_a, v_a, w_b, m_b, v_b, nw_a, nm_a, nv_a, nw_b, nm_b, nv_b) = refs[30:42]
    local_sem, send_sem, recv_sem = refs[42:45]

    me = lax.axis_index("dp")
    c, z, y = lax.rem(me, C), lax.rem(lax.div(me, C), Z), lax.div(me, C * Z)
    other_c, other_y = 1 - c, 1 - y
    mate = {"dp": me + 1 - 2 * c}
    across = {"dp": me + (1 - 2 * y) * (Z * C)}
    right, left = {"dp": me + C}, {"dp": me - C}
    n = 6 * split
    big, small = 3 * tiles // 5 // split, 2 * tiles // 5 // split

    barrier = pltpu.get_barrier_semaphore()
    pl.semaphore_signal(barrier, inc=1, device_id=mate, device_id_type=MESH)
    pl.semaphore_signal(barrier, inc=1, device_id=across, device_id_type=MESH)

    @pl.when(z > 0)
    def _():
        pl.semaphore_signal(barrier, inc=1, device_id=left, device_id_type=MESH)

    @pl.when(z < Z - 1)
    def _():
        pl.semaphore_signal(barrier, inc=1, device_id=right, device_id_type=MESH)

    for ref in (l_a, l_b):
        ref[:, 0] = jnp.zeros_like(ref[:, 0])
    for ref in (r_a, r_b):
        ref[:, Z - 1] = jnp.zeros_like(ref[:, Z - 1])

    @pl.when((z > 0) & (z < Z - 1))
    def _():
        pl.semaphore_wait(barrier, 4)

    @pl.when((z == 0) | (z == Z - 1))
    def _():
        pl.semaphore_wait(barrier, 3)

    def remote(kind, q, src, dst, device):
        slot = lax.rem(q, SENDS)
        return pltpu.make_async_remote_copy(
            src_ref=src, dst_ref=dst, send_sem=send_sem.at[kind, slot], recv_sem=recv_sem.at[kind, slot], device_id=device, device_id_type=MESH
        )

    def local(kind, q, src, dst):
        return pltpu.make_async_copy(src, dst, local_sem.at[kind, lax.rem(q, SENDS)])

    def f(ref):
        return ref[...].astype(F32)

    def where(q):
        return lax.div(q, split), lax.rem(q, split)

    def by_weight(ml, act):
        for a in range(3):

            @pl.when(lax.div(ml, 2) == a)
            def _(a=a):
                act(a, lax.rem(ml, 2))

    class Part:
        def __init__(self, which):
            self.which = which
            self.base = 12 * which
            self.count = (big, small)[which]
            self.first = (0, big * split)[which]
            self.own, self.part, self.ry, self.rl, self.rr, self.sy, self.sl, self.sr = (
                (own_a, part_a, y_a, l_a, r_a, sy_a, sl_a, sr_a),
                (own_b, part_b, y_b, l_b, r_b, sy_b, sl_b, sr_b),
            )[which]
            self.w, self.m, self.v, self.nw, self.nm, self.nv = (
                (w_a, m_a, v_a, nw_a, nm_a, nv_a),
                (w_b, m_b, v_b, nw_b, nm_b, nv_b),
            )[which]

        def at(self, q):
            return pl.ds(self.first + lax.rem(q, split) * self.count, self.count)

        def remote(self, kind, q, src, dst, device):
            return remote(self.base + kind, q, src, dst, device)

        def local(self, kind, q, src, dst):
            return local(7 * self.which + kind, q, src, dst)

        def terms(self, q):
            slot = lax.rem(q, RING)

            def act(a, layer):
                self.remote(0, q, g[a].at[layer, :, :, other_c, self.at(q)], self.part.at[slot], mate).start()
                self.local(0, q, g[a].at[layer, :, :, c, self.at(q)], self.own.at[slot]).start()

            by_weight(where(q)[0], act)

        def terms_wait(self, q):
            slot = lax.rem(q, RING)
            self.local(0, q, self.own.at[slot], self.own.at[slot]).wait()
            self.remote(0, q, self.part.at[slot], self.part.at[slot], mate).wait_recv()

        def terms_sent(self, q):
            slot = lax.rem(q, RING)
            self.remote(0, q, self.part.at[slot], self.part.at[slot], mate).wait_send()

        def z_block(self, slot, j):
            raise NotImplementedError

        def z_send(self, q, h):
            slot, to = lax.rem(q, RING), lax.rem(q, SENDS)

            @pl.when(z == h - 1)
            def _():
                for j in range(h, Z):
                    self.z_sum(slot, j, self.sr.at[to, j], self.rl if h > 1 else None)
                self.remote(2, q, self.sr.at[to, h:Z], self.rl.at[slot, h:Z], right).start()

            @pl.when(z == Z - h)
            def _():
                for j in range(Z - h):
                    self.z_sum(slot, j, self.sl.at[to, j], self.rr if h > 1 else None)
                self.remote(3, q, self.sl.at[to, 0 : Z - h], self.rr.at[slot, 0 : Z - h], left).start()

        def z_wait(self, q, h):
            slot = lax.rem(q, RING)

            @pl.when(z == h)
            def _():
                self.remote(2, q, self.rl.at[slot, h:Z], self.rl.at[slot, h:Z], right).wait_recv()

            @pl.when(z == Z - 1 - h)
            def _():
                self.remote(3, q, self.rr.at[slot, 0 : Z - h], self.rr.at[slot, 0 : Z - h], left).wait_recv()

        def z_sent(self, q, h):
            to = lax.rem(q, SENDS)

            @pl.when(z == h - 1)
            def _():
                self.remote(2, q, self.sr.at[to, h:Z], self.sr.at[to, h:Z], right).wait_send()

            @pl.when(z == Z - h)
            def _():
                self.remote(3, q, self.sl.at[to, 0 : Z - h], self.sl.at[to, 0 : Z - h], left).wait_send()

        def state(self, q):
            slot = lax.rem(q, SENDS)

            def act(a, layer):
                self.local(1, q, w[a].at[layer, y, z, c, self.at(q)], self.w.at[slot]).start()
                self.local(2, q, m[a].at[layer, self.at(q)], self.m.at[slot]).start()
                self.local(3, q, v[a].at[layer, self.at(q)], self.v.at[slot]).start()

            by_weight(where(q)[0], act)

        def step(self, q, total):
            slot = lax.rem(q, SENDS)
            self.local(1, q, self.w.at[slot], self.w.at[slot]).wait()
            self.local(2, q, self.m.at[slot], self.m.at[slot]).wait()
            self.local(3, q, self.v.at[slot], self.v.at[slot]).wait()
            grad = total.astype(BF16).astype(F32)
            weight = f(self.w.at[slot])
            new_m = 0.9 * self.m[slot] + 0.1 * grad
            new_v = 0.95 * self.v[slot] + 0.05 * grad * grad
            self.nm[slot] = new_m
            self.nv[slot] = new_v
            self.nw[slot] = (weight - 0.02 * (new_m * lax.rsqrt(new_v + 1e-8) + 0.1 * weight)).astype(BF16)
            ml, _ = where(q)
            self.local(4, q, self.nw.at[slot], out.at[ml, y, z, c, self.at(q)]).start()
            self.local(5, q, self.nm.at[slot], moments.at[0, ml, self.at(q)]).start()
            self.local(6, q, self.nv.at[slot], moments.at[1, ml, self.at(q)]).start()

        def weight_stored(self, q):
            slot = lax.rem(q, SENDS)
            self.local(4, q, self.nw.at[slot], self.nw.at[slot]).wait()

        def moments_stored(self, q):
            slot = lax.rem(q, SENDS)
            self.local(5, q, self.nm.at[slot], self.nm.at[slot]).wait()
            self.local(6, q, self.nv.at[slot], self.nv.at[slot]).wait()

        def spread(self, q, h, src=None):
            @pl.when((z >= h) & (z < Z - 1))
            def _():
                dst = self.row(q, z - h)
                self.remote(5 + h, q, dst if src is None else src, dst, right).start()

            @pl.when((z + h < Z) & (z > 0))
            def _():
                dst = self.row(q, z + h)
                self.remote(8 + h, q, dst if src is None else src, dst, left).start()

        def spread_wait(self, q, h):
            @pl.when(z > h)
            def _():
                ref = self.row(q, z - h - 1)
                self.remote(5 + h, q, ref, ref, right).wait_recv()

            @pl.when(z + h + 1 < Z)
            def _():
                ref = self.row(q, z + h + 1)
                self.remote(8 + h, q, ref, ref, left).wait_recv()

        def spread_sent(self, q, h):
            @pl.when((z >= h) & (z < Z - 1))
            def _():
                ref = self.row(q, z - h)
                self.remote(5 + h, q, ref, ref, right).wait_send()

            @pl.when((z + h < Z) & (z > 0))
            def _():
                ref = self.row(q, z + h)
                self.remote(8 + h, q, ref, ref, left).wait_send()

        def share(self, q):
            ref = out.at[where(q)[0], :, :, c, self.at(q)]
            self.remote(11, q, ref, ref, mate).start()

        def share_wait(self, q):
            ref = out.at[where(q)[0], :, :, other_c, self.at(q)]
            self.remote(11, q, ref, ref, mate).wait_recv()

        def share_sent(self, q):
            ref = out.at[where(q)[0], :, :, c, self.at(q)]
            self.remote(11, q, ref, ref, mate).wait_send()

    class YFirst(Part):
        def row(self, q, j):
            return out.at[where(q)[0], y, j, c, self.at(q)]

        def z_sum(self, slot, j, to, more):
            total = f(self.own.at[slot, y, j]) + f(self.part.at[slot, y, j]) + f(self.ry.at[slot, j])
            to[...] = (total if more is None else total + f(more.at[slot, j])).astype(BF16)

        def y_send(self, q):
            slot, to = lax.rem(q, RING), lax.rem(q, SENDS)
            for j in range(Z):
                self.sy[to, j] = (f(self.own.at[slot, other_y, j]) + f(self.part.at[slot, other_y, j])).astype(BF16)
            self.remote(1, q, self.sy.at[to], self.ry.at[slot], across).start()

        def y_wait(self, q):
            slot = lax.rem(q, RING)
            self.remote(1, q, self.ry.at[slot], self.ry.at[slot], across).wait_recv()

        def y_sent(self, q):
            to = lax.rem(q, SENDS)
            self.remote(1, q, self.sy.at[to], self.sy.at[to], across).wait_send()

        def finish(self, q):
            slot = lax.rem(q, RING)
            total = f(self.own.at[slot, y, z]) + f(self.part.at[slot, y, z]) + f(self.ry.at[slot, z])
            self.step(q, total + f(self.rl.at[slot, z]) + f(self.rr.at[slot, z]))
            self.spread(q, 0, self.nw.at[lax.rem(q, SENDS)])

        def y_spread(self, q):
            ref = out.at[where(q)[0], y, :, c, self.at(q)]
            self.remote(4, q, ref, ref, across).start()

        def y_spread_wait(self, q):
            ref = out.at[where(q)[0], other_y, :, c, self.at(q)]
            self.remote(4, q, ref, ref, across).wait_recv()

        def y_spread_sent(self, q):
            ref = out.at[where(q)[0], y, :, c, self.at(q)]
            self.remote(4, q, ref, ref, across).wait_send()

    class ZFirst(Part):
        def row(self, q, j):
            return out.at[where(q)[0], :, j, c, self.at(q)]

        def z_sum(self, slot, j, to, more):
            for i in range(Y):
                total = f(self.own.at[slot, i, j]) + f(self.part.at[slot, i, j])
                to[i] = (total if more is None else total + f(more.at[slot, j, i])).astype(BF16)

        def column(self, slot, i):
            total = f(self.own.at[slot, i, z]) + f(self.part.at[slot, i, z])
            return total + f(self.rl.at[slot, z, i]) + f(self.rr.at[slot, z, i])

        def y_send(self, q):
            slot, to = lax.rem(q, RING), lax.rem(q, SENDS)
            self.sy[to] = self.column(slot, other_y).astype(BF16)
            self.remote(1, q, self.sy.at[to], self.ry.at[slot], across).start()

        def y_wait(self, q):
            slot = lax.rem(q, RING)
            self.remote(1, q, self.ry.at[slot], self.ry.at[slot], across).wait_recv()

        def y_sent(self, q):
            to = lax.rem(q, SENDS)
            self.remote(1, q, self.sy.at[to], self.sy.at[to], across).wait_send()

        def finish(self, q):
            slot = lax.rem(q, RING)
            self.step(q, self.column(slot, y) + f(self.ry.at[slot]))
            ref = out.at[where(q)[0], y, z, c, self.at(q)]
            self.remote(4, q, self.nw.at[lax.rem(q, SENDS)], ref, across).start()

        def y_spread_wait(self, q):
            ref = out.at[where(q)[0], other_y, z, c, self.at(q)]
            self.remote(4, q, ref, ref, across).wait_recv()

        def y_spread_sent(self, q):
            ref = out.at[where(q)[0], y, z, c, self.at(q)]
            self.remote(4, q, ref, ref, across).wait_send()

    a, b = YFirst(0), ZFirst(1)

    def iteration(t, _):
        def at(stage, *acts):
            q = t - stage

            @pl.when((q >= 0) & (q < n))
            def _():
                for act in acts:
                    act(q)

        def hop(act, h):
            return lambda q: act(q, h)

        at(0, a.terms, b.terms)
        at(0 + DRAIN, a.terms_sent, b.terms_sent)
        at(1 + DRAIN, a.y_sent, hop(b.z_sent, 1))
        at(2 + DRAIN, hop(a.z_sent, 1), hop(b.z_sent, 2))
        at(3 + DRAIN, hop(a.z_sent, 2), hop(b.z_sent, 3))
        at(4 + DRAIN, hop(a.z_sent, 3), b.y_sent)
        at(5 + DRAIN, hop(a.spread_sent, 0), b.y_spread_sent, a.moments_stored, b.moments_stored)
        at(6 + DRAIN, hop(a.spread_sent, 1), hop(b.spread_sent, 0))
        at(7 + DRAIN, hop(a.spread_sent, 2), hop(b.spread_sent, 1))
        at(8 + DRAIN, a.y_spread_sent, hop(b.spread_sent, 2))
        at(9 + DRAIN, a.share_sent, b.share_sent)
        at(3, a.state, b.state)
        at(1, a.terms_wait, a.y_send)
        at(8, hop(a.spread_wait, 2), a.y_spread)
        at(7, hop(a.spread_wait, 1), hop(a.spread, 2))
        at(6, a.weight_stored, hop(a.spread_wait, 0), hop(a.spread, 1))
        at(2, a.y_wait, hop(a.z_send, 1))
        at(3, hop(a.z_wait, 1), hop(a.z_send, 2))
        at(4, hop(a.z_wait, 2), hop(a.z_send, 3))
        at(5, hop(a.z_wait, 3), a.finish)
        at(9, a.y_spread_wait, a.share)
        at(1, b.terms_wait, hop(b.z_send, 1))
        at(8, hop(b.spread_wait, 1), hop(b.spread, 2))
        at(7, hop(b.spread_wait, 0), hop(b.spread, 1))
        at(6, b.weight_stored, b.y_spread_wait, hop(b.spread, 0))
        at(2, hop(b.z_wait, 1), hop(b.z_send, 2))
        at(3, hop(b.z_wait, 2), hop(b.z_send, 3))
        at(4, hop(b.z_wait, 3), b.y_send)
        at(5, b.y_wait, b.finish)
        at(9, hop(b.spread_wait, 2), b.share)
        at(10, a.share_wait, b.share_wait)
        return 0

    lax.fori_loop(0, n + LAST, iteration, 0)


def to_tiles(x, lead):
    *head, rows, columns = x.shape
    k = len(head)
    x = x.reshape(*head, rows // 8, 8, columns // 128, 128).transpose(*range(k), k, k + 2, k + 1, k + 3)
    return x.reshape(*lead, -1, 8, 128)


def from_tiles(x, shape):
    *head, rows, columns = shape
    k = len(head)
    x = x.reshape(*head, rows // 8, columns // 128, 8, 128).transpose(*range(k), k, k + 2, k + 1, k + 3)
    return x.reshape(shape)


def solution(mesh, split=SPLIT, options=None):
    def step(*arrays):
        terms, weights, m, v = (arrays[i : i + 3] for i in (0, 3, 6, 9))
        g = [to_tiles(t[0], (2, Y, Z, C)) for t in terms]
        w = [to_tiles(t, (2, Y, Z, C)) for t in weights]
        state = [to_tiles(t, (2,)) for t in (*m, *v)]
        tiles = state[0].shape[1]
        tile = (8, 128)

        def scratch(count):
            ring, sends = (RING,), (SENDS,)
            return ring, sends, (count, *tile)

        def buffers(count, line):
            one = (count, *tile)
            blocks = [(RING, Y, Z, *one)] * 2 + [(RING, *((Z,) if line == () else ()), *one)] + [(RING, Z, *line, *one)] * 2
            sent = [(SENDS, *((Z,) if line == () else ()), *one)] + [(SENDS, Z, *line, *one)] * 2
            return [pltpu.VMEM(shape, BF16) for shape in blocks + sent]

        big, small = 3 * tiles // 5 // split, 2 * tiles // 5 // split
        held = []
        for count in (big, small):
            held += [pltpu.VMEM((SENDS, count, *tile), t) for t in (BF16, F32, F32)]
        for count in (big, small):
            held += [pltpu.VMEM((SENDS, count, *tile), t) for t in (BF16, F32, F32)]
        out, moments = pl.pallas_call(
            functools.partial(kernel, split, tiles),
            out_shape=(
                jax.ShapeDtypeStruct((6, Y, Z, C, tiles, *tile), BF16),
                jax.ShapeDtypeStruct((2, 6, tiles, *tile), F32),
            ),
            in_specs=[pl.BlockSpec(memory_space=pl.ANY)] * 12,
            out_specs=(pl.BlockSpec(memory_space=pl.ANY),) * 2,
            scratch_shapes=[
                *buffers(big, ()),
                *buffers(small, (Y,)),
                *held,
                pltpu.SemaphoreType.DMA((14, SENDS)),
                pltpu.SemaphoreType.DMA((24, SENDS)),
                pltpu.SemaphoreType.DMA((24, SENDS)),
            ],
            compiler_params=pltpu.CompilerParams(collective_id=0, has_side_effects=True),
            name="step",
        )(*g, *w, *state)
        new = [from_tiles(out[2 * i : 2 * i + 2], t.shape) for i, t in enumerate(weights)]
        new_m = [from_tiles(moments[0, 2 * i : 2 * i + 2], t.shape) for i, t in enumerate(m)]
        new_v = [from_tiles(moments[1, 2 * i : 2 * i + 2], t.shape) for i, t in enumerate(v)]
        return (*new, *new_m, *new_v)

    all_of, cut = P(None, None, None), P(None, "dp", None)
    return jax.shard_map(
        step,
        mesh=mesh,
        in_specs=(P(("rep", "dp"), None, None, None),) * 3 + (all_of,) * 3 + (cut,) * 6,
        out_specs=(P("rep", None, None),) * 3 + (P("rep", "dp", None),) * 6,
        check_vma=False,
    )
```

```python
import functools

import jax
import jax.numpy as jnp
from jax import lax
from jax.experimental import pallas as pl
from jax.experimental.pallas import tpu as pltpu
from jax.sharding import PartitionSpec as P

MESH = pl.DeviceIdType.MESH
F32, BF16 = jnp.float32, jnp.bfloat16
Y, Z, C = 2, 4, 2
SPLIT = 16
RING = 8
SENDS = 4
DRAIN = 2
LAST = 10 + DRAIN
FAR = 3
DEPTH = 4
VMEM_BYTES = 67_043_328


def kernel(split, tiles, *refs):
    g, w, m, v = (refs[i : i + 3] for i in (0, 3, 6, 9))
    far, near, moments = refs[12:15]
    (own_a, part_a, y_a, l_a, r_a, sy_a, sl_a, sr_a, own_b, part_b, y_b, l_b, r_b, sy_b, sl_b, sr_b) = refs[15:31]
    (w_a, m_a, v_a, nw_a, w_b, m_b, v_b, nw_b) = refs[31:39]
    local_sem, send_sem, recv_sem = refs[39:42]

    me = lax.axis_index("dp")
    c, z, y = lax.rem(me, C), lax.rem(lax.div(me, C), Z), lax.div(me, C * Z)
    other_c, other_y = 1 - c, 1 - y
    mate = {"dp": me + 1 - 2 * c}
    across = {"dp": me + (1 - 2 * y) * (Z * C)}
    right, left = {"dp": me + C}, {"dp": me - C}
    n = 6 * split
    big, small = 3 * tiles // 5 // split, 2 * tiles // 5 // split

    barrier = pltpu.get_barrier_semaphore()
    pl.semaphore_signal(barrier, inc=1, device_id=mate, device_id_type=MESH)
    pl.semaphore_signal(barrier, inc=1, device_id=across, device_id_type=MESH)

    @pl.when(z > 0)
    def _():
        pl.semaphore_signal(barrier, inc=1, device_id=left, device_id_type=MESH)

    @pl.when(z < Z - 1)
    def _():
        pl.semaphore_signal(barrier, inc=1, device_id=right, device_id_type=MESH)

    for ref in (l_a, l_b):
        ref[:, 0] = jnp.zeros_like(ref[:, 0])
    for ref in (r_a, r_b):
        ref[:, Z - 1] = jnp.zeros_like(ref[:, Z - 1])

    @pl.when((z > 0) & (z < Z - 1))
    def _():
        pl.semaphore_wait(barrier, 4)

    @pl.when((z == 0) | (z == Z - 1))
    def _():
        pl.semaphore_wait(barrier, 3)

    def remote(kind, q, src, dst, device):
        slot = lax.rem(q, SENDS)
        return pltpu.make_async_remote_copy(
            src_ref=src, dst_ref=dst, send_sem=send_sem.at[kind, slot], recv_sem=recv_sem.at[kind, slot], device_id=device, device_id_type=MESH
        )

    def local(kind, q, src, dst):
        return pltpu.make_async_copy(src, dst, local_sem.at[kind, lax.rem(q, SENDS)])

    def f(ref):
        return ref[...].astype(F32)

    def where(q):
        return lax.div(q, split), lax.rem(q, split)

    def by_weight(ml, act):
        for a in range(3):

            @pl.when(lax.div(ml, 2) == a)
            def _(a=a):
                act(a, lax.rem(ml, 2))

    def placed(q, act):
        ml = lax.div(q, split)

        @pl.when(ml < FAR)
        def _():
            act(far.at[ml])

        @pl.when(ml >= FAR)
        def _():
            act(near.at[ml - FAR])

    class Part:
        def __init__(self, which):
            self.which = which
            self.base = 12 * which
            self.count = (big, small)[which]
            self.first = (0, big * split)[which]
            self.own, self.part, self.ry, self.rl, self.rr, self.sy, self.sl, self.sr = (
                (own_a, part_a, y_a, l_a, r_a, sy_a, sl_a, sr_a),
                (own_b, part_b, y_b, l_b, r_b, sy_b, sl_b, sr_b),
            )[which]
            self.w, self.m, self.v, self.nw = ((w_a, m_a, v_a, nw_a), (w_b, m_b, v_b, nw_b))[which]

        def at(self, q):
            return pl.ds(self.first + lax.rem(q, split) * self.count, self.count)

        def remote(self, kind, q, src, dst, device):
            return remote(self.base + kind, q, src, dst, device)

        def local(self, kind, q, src, dst):
            return local(5 * self.which + kind, q, src, dst)

        def terms(self, q):
            slot = lax.rem(q, RING)

            def act(a, layer):
                self.remote(0, q, g[a].at[layer, :, :, other_c, self.at(q)], self.part.at[slot], mate).start()
                self.local(0, q, g[a].at[layer, :, :, c, self.at(q)], self.own.at[slot]).start()

            by_weight(where(q)[0], act)

        def terms_wait(self, q):
            slot = lax.rem(q, RING)
            self.local(0, q, self.own.at[slot], self.own.at[slot]).wait()
            self.remote(0, q, self.part.at[slot], self.part.at[slot], mate).wait_recv()

        def terms_sent(self, q):
            slot = lax.rem(q, RING)
            self.remote(0, q, self.part.at[slot], self.part.at[slot], mate).wait_send()

        def z_block(self, slot, j):
            raise NotImplementedError

        def z_send(self, q, h):
            slot, to = lax.rem(q, RING), lax.rem(q, SENDS)

            @pl.when(z == h - 1)
            def _():
                for j in range(h, Z):
                    self.z_sum(slot, j, self.sr.at[to, j], self.rl if h > 1 else None)
                self.remote(2, q, self.sr.at[to, h:Z], self.rl.at[slot, h:Z], right).start()

            @pl.when(z == Z - h)
            def _():
                for j in range(Z - h):
                    self.z_sum(slot, j, self.sl.at[to, j], self.rr if h > 1 else None)
                self.remote(3, q, self.sl.at[to, 0 : Z - h], self.rr.at[slot, 0 : Z - h], left).start()

        def z_wait(self, q, h):
            slot = lax.rem(q, RING)

            @pl.when(z == h)
            def _():
                self.remote(2, q, self.rl.at[slot, h:Z], self.rl.at[slot, h:Z], right).wait_recv()

            @pl.when(z == Z - 1 - h)
            def _():
                self.remote(3, q, self.rr.at[slot, 0 : Z - h], self.rr.at[slot, 0 : Z - h], left).wait_recv()

        def z_sent(self, q, h):
            to = lax.rem(q, SENDS)

            @pl.when(z == h - 1)
            def _():
                self.remote(2, q, self.sr.at[to, h:Z], self.sr.at[to, h:Z], right).wait_send()

            @pl.when(z == Z - h)
            def _():
                self.remote(3, q, self.sl.at[to, 0 : Z - h], self.sl.at[to, 0 : Z - h], left).wait_send()

        def state(self, q):
            slot = lax.rem(q, SENDS)

            def act(a, layer):
                self.local(1, q, w[a].at[layer, y, z, c, self.at(q)], self.w.at[slot]).start()
                self.local(2, q, m[a].at[layer, self.at(q)], self.m.at[slot]).start()
                self.local(3, q, v[a].at[layer, self.at(q)], self.v.at[slot]).start()

            by_weight(where(q)[0], act)

        def step(self, q, total):
            slot = lax.rem(q, SENDS)
            self.local(1, q, self.w.at[slot], self.w.at[slot]).wait()
            self.local(2, q, self.m.at[slot], self.m.at[slot]).wait()
            self.local(3, q, self.v.at[slot], self.v.at[slot]).wait()
            grad = total.astype(BF16).astype(F32)
            weight = f(self.w.at[slot])
            new_m = 0.9 * self.m[slot] + 0.1 * grad
            new_v = 0.95 * self.v[slot] + 0.05 * grad * grad
            ml, _ = where(q)
            moments[0, ml, self.at(q)] = new_m
            moments[1, ml, self.at(q)] = new_v
            new_w = (weight - 0.02 * (new_m * lax.rsqrt(new_v + 1e-8) + 0.1 * weight)).astype(BF16)
            self.nw[slot] = new_w

            @pl.when(ml < FAR)
            def _():
                self.local(4, q, self.nw.at[slot], far.at[ml, y, z, c, self.at(q)]).start()

            @pl.when(ml >= FAR)
            def _():
                near[ml - FAR, y, z, c, self.at(q)] = new_w

        def weight_stored(self, q):
            slot = lax.rem(q, SENDS)

            @pl.when(where(q)[0] < FAR)
            def _():
                self.local(4, q, self.nw.at[slot], self.nw.at[slot]).wait()

        def spread(self, q, h, src=None):
            def act(o):
                @pl.when((z >= h) & (z < Z - 1))
                def _():
                    dst = self.row(o, q, z - h)
                    self.remote(5 + h, q, dst if src is None else src, dst, right).start()

                @pl.when((z + h < Z) & (z > 0))
                def _():
                    dst = self.row(o, q, z + h)
                    self.remote(8 + h, q, dst if src is None else src, dst, left).start()

            placed(q, act)

        def spread_wait(self, q, h):
            def act(o):
                @pl.when(z > h)
                def _():
                    ref = self.row(o, q, z - h - 1)
                    self.remote(5 + h, q, ref, ref, right).wait_recv()

                @pl.when(z + h + 1 < Z)
                def _():
                    ref = self.row(o, q, z + h + 1)
                    self.remote(8 + h, q, ref, ref, left).wait_recv()

            placed(q, act)

        def spread_sent(self, q, h):
            def act(o):
                @pl.when((z >= h) & (z < Z - 1))
                def _():
                    ref = self.row(o, q, z - h)
                    self.remote(5 + h, q, ref, ref, right).wait_send()

                @pl.when((z + h < Z) & (z > 0))
                def _():
                    ref = self.row(o, q, z + h)
                    self.remote(8 + h, q, ref, ref, left).wait_send()

            placed(q, act)

        def share(self, q):
            def act(o):
                ref = o.at[:, :, c, self.at(q)]
                self.remote(11, q, ref, ref, mate).start()

            placed(q, act)

        def share_wait(self, q):
            def act(o):
                ref = o.at[:, :, other_c, self.at(q)]
                self.remote(11, q, ref, ref, mate).wait_recv()

            placed(q, act)

        def share_sent(self, q):
            def act(o):
                ref = o.at[:, :, c, self.at(q)]
                self.remote(11, q, ref, ref, mate).wait_send()

            placed(q, act)

    class YFirst(Part):
        def row(self, o, q, j):
            return o.at[y, j, c, self.at(q)]

        def z_sum(self, slot, j, to, more):
            total = f(self.own.at[slot, y, j]) + f(self.part.at[slot, y, j]) + f(self.ry.at[slot, j])
            to[...] = (total if more is None else total + f(more.at[slot, j])).astype(BF16)

        def y_send(self, q):
            slot, to = lax.rem(q, RING), lax.rem(q, SENDS)
            for j in range(Z):
                self.sy[to, j] = (f(self.own.at[slot, other_y, j]) + f(self.part.at[slot, other_y, j])).astype(BF16)
            self.remote(1, q, self.sy.at[to], self.ry.at[slot], across).start()

        def y_wait(self, q):
            slot = lax.rem(q, RING)
            self.remote(1, q, self.ry.at[slot], self.ry.at[slot], across).wait_recv()

        def y_sent(self, q):
            to = lax.rem(q, SENDS)
            self.remote(1, q, self.sy.at[to], self.sy.at[to], across).wait_send()

        def finish(self, q):
            slot = lax.rem(q, RING)
            total = f(self.own.at[slot, y, z]) + f(self.part.at[slot, y, z]) + f(self.ry.at[slot, z])
            self.step(q, total + f(self.rl.at[slot, z]) + f(self.rr.at[slot, z]))
            self.spread(q, 0, self.nw.at[lax.rem(q, SENDS)])

        def y_spread(self, q):
            def act(o):
                ref = o.at[y, :, c, self.at(q)]
                self.remote(4, q, ref, ref, across).start()

            placed(q, act)

        def y_spread_wait(self, q):
            def act(o):
                ref = o.at[other_y, :, c, self.at(q)]
                self.remote(4, q, ref, ref, across).wait_recv()

            placed(q, act)

        def y_spread_sent(self, q):
            def act(o):
                ref = o.at[y, :, c, self.at(q)]
                self.remote(4, q, ref, ref, across).wait_send()

            placed(q, act)

    class ZFirst(Part):
        def row(self, o, q, j):
            return o.at[:, j, c, self.at(q)]

        def z_sum(self, slot, j, to, more):
            for i in range(Y):
                total = f(self.own.at[slot, i, j]) + f(self.part.at[slot, i, j])
                to[i] = (total if more is None else total + f(more.at[slot, j, i])).astype(BF16)

        def column(self, slot, i):
            total = f(self.own.at[slot, i, z]) + f(self.part.at[slot, i, z])
            return total + f(self.rl.at[slot, z, i]) + f(self.rr.at[slot, z, i])

        def y_send(self, q):
            slot, to = lax.rem(q, RING), lax.rem(q, SENDS)
            self.sy[to] = self.column(slot, other_y).astype(BF16)
            self.remote(1, q, self.sy.at[to], self.ry.at[slot], across).start()

        def y_wait(self, q):
            slot = lax.rem(q, RING)
            self.remote(1, q, self.ry.at[slot], self.ry.at[slot], across).wait_recv()

        def y_sent(self, q):
            to = lax.rem(q, SENDS)
            self.remote(1, q, self.sy.at[to], self.sy.at[to], across).wait_send()

        def finish(self, q):
            slot = lax.rem(q, RING)
            self.step(q, self.column(slot, y) + f(self.ry.at[slot]))

            def act(o):
                self.remote(4, q, self.nw.at[lax.rem(q, SENDS)], o.at[y, z, c, self.at(q)], across).start()

            placed(q, act)

        def y_spread_wait(self, q):
            def act(o):
                ref = o.at[other_y, z, c, self.at(q)]
                self.remote(4, q, ref, ref, across).wait_recv()

            placed(q, act)

        def y_spread_sent(self, q):
            def act(o):
                ref = o.at[y, z, c, self.at(q)]
                self.remote(4, q, ref, ref, across).wait_send()

            placed(q, act)

    a, b = YFirst(0), ZFirst(1)

    def iteration(t, _):
        def at(stage, *acts):
            q = t - stage

            @pl.when((q >= 0) & (q < n))
            def _():
                for act in acts:
                    act(q)

        def hop(act, h):
            return lambda q: act(q, h)

        at(0, a.terms, b.terms)
        at(0 + DRAIN, a.terms_sent, b.terms_sent)
        at(1 + DRAIN, a.y_sent, hop(b.z_sent, 1))
        at(2 + DRAIN, hop(a.z_sent, 1), hop(b.z_sent, 2))
        at(3 + DRAIN, hop(a.z_sent, 2), hop(b.z_sent, 3))
        at(4 + DRAIN, hop(a.z_sent, 3), b.y_sent)
        at(5 + DRAIN, hop(a.spread_sent, 0), b.y_spread_sent)
        at(6 + DRAIN, hop(a.spread_sent, 1), hop(b.spread_sent, 0))
        at(7 + DRAIN, hop(a.spread_sent, 2), hop(b.spread_sent, 1))
        at(8 + DRAIN, a.y_spread_sent, hop(b.spread_sent, 2))
        at(9 + DRAIN, a.share_sent, b.share_sent)
        at(3, a.state, b.state)
        at(1, a.terms_wait, a.y_send)
        at(8, hop(a.spread_wait, 2), a.y_spread)
        at(7, hop(a.spread_wait, 1), hop(a.spread, 2))
        at(6, a.weight_stored, hop(a.spread_wait, 0), hop(a.spread, 1))
        at(2, a.y_wait, hop(a.z_send, 1))
        at(3, hop(a.z_wait, 1), hop(a.z_send, 2))
        at(4, hop(a.z_wait, 2), hop(a.z_send, 3))
        at(5, hop(a.z_wait, 3), a.finish)
        at(9, a.y_spread_wait, a.share)
        at(1, b.terms_wait, hop(b.z_send, 1))
        at(8, hop(b.spread_wait, 1), hop(b.spread, 2))
        at(7, hop(b.spread_wait, 0), hop(b.spread, 1))
        at(6, b.weight_stored, b.y_spread_wait, hop(b.spread, 0))
        at(2, hop(b.z_wait, 1), hop(b.z_send, 2))
        at(3, hop(b.z_wait, 2), hop(b.z_send, 3))
        at(4, hop(b.z_wait, 3), b.y_send)
        at(5, b.y_wait, b.finish)
        at(9, hop(b.spread_wait, 2), b.share)
        at(10, a.share_wait, b.share_wait)
        return 0

    lax.fori_loop(0, n + LAST, iteration, 0)


def store(far, near, moments, *refs):
    new, states, (line, read_sem, write_sem, held_sem) = refs[:3], refs[3:9], refs[9:]
    pieces = [(ml, j) for ml in range(FAR) for j in range(Y * Z)]

    def read(i):
        ml, j = pieces[i]
        return pltpu.make_async_copy(far.at[ml, j // Z, j % Z], line.at[i % DEPTH], read_sem.at[i % DEPTH])

    def write(i):
        ml, j = pieces[i]
        return pltpu.make_async_copy(line.at[i % DEPTH], new[ml // 2].at[ml % 2, j // Z, j % Z], write_sem.at[i % DEPTH])

    held = [(near.at[ml - FAR], new[ml // 2].at[ml % 2]) for ml in range(FAR, 6)]
    held += [(moments.at[i // 3, 2 * (i % 3) : 2 * (i % 3) + 2], states[i]) for i in range(6)]
    held = [pltpu.make_async_copy(src, dst, held_sem.at[i]) for i, (src, dst) in enumerate(held)]
    for i in range(DEPTH):
        read(i).start()
    for copy in held:
        copy.start()
    for i in range(len(pieces)):
        read(i).wait()
        write(i).start()
        if i >= 1 and i - 1 + DEPTH < len(pieces):
            write(i - 1).wait()
            read(i - 1 + DEPTH).start()
    for i in range(len(pieces) - DEPTH, len(pieces)):
        write(i).wait()
    for copy in held:
        copy.wait()


def to_tiles(x, lead):
    *head, rows, columns = x.shape
    k = len(head)
    x = x.reshape(*head, rows // 8, 8, columns // 128, 128).transpose(*range(k), k, k + 2, k + 1, k + 3)
    return x.reshape(*lead, -1, 8, 128)


def from_tiles(x, shape):
    *head, rows, columns = shape
    k = len(head)
    x = x.reshape(*head, rows // 8, columns // 128, 8, 128).transpose(*range(k), k, k + 2, k + 1, k + 3)
    return x.reshape(shape)


def solution(mesh, split=SPLIT):
    def step(*arrays):
        terms, weights, m, v = (arrays[i : i + 3] for i in (0, 3, 6, 9))
        g = [to_tiles(t[0], (2, Y, Z, C)) for t in terms]
        w = [to_tiles(t, (2, Y, Z, C)) for t in weights]
        state = [to_tiles(t, (2,)) for t in (*m, *v)]
        tiles = state[0].shape[1]
        tile = (8, 128)
        limit = VMEM_BYTES - 1024 * tiles * (2 * Y * Z * C * (6 - FAR) + 4 * 2 * 6)

        def buffers(count, line):
            one = (count, *tile)
            blocks = [(RING, Y, Z, *one)] * 2 + [(RING, *((Z,) if line == () else ()), *one)] + [(RING, Z, *line, *one)] * 2
            sent = [(SENDS, *((Z,) if line == () else ()), *one)] + [(SENDS, Z, *line, *one)] * 2
            return [pltpu.VMEM(shape, BF16) for shape in blocks + sent]

        big, small = 3 * tiles // 5 // split, 2 * tiles // 5 // split
        held = [pltpu.VMEM((SENDS, count, *tile), t) for count in (big, small) for t in (BF16, F32, F32, BF16)]
        whole = (Y, Z, C, tiles, *tile)
        hbm, vmem = pl.BlockSpec(memory_space=pltpu.HBM), pl.BlockSpec(memory_space=pltpu.VMEM)
        far, near, moments = pl.pallas_call(
            functools.partial(kernel, split, tiles),
            out_shape=(pltpu.HBM((FAR, *whole), BF16), pltpu.VMEM((6 - FAR, *whole), BF16), pltpu.VMEM((2, 6, tiles, *tile), F32)),
            in_specs=[pl.BlockSpec(memory_space=pl.ANY)] * 12,
            out_specs=(hbm, vmem, vmem),
            scratch_shapes=[
                *buffers(big, ()),
                *buffers(small, (Y,)),
                *held,
                pltpu.SemaphoreType.DMA((10, SENDS)),
                pltpu.SemaphoreType.DMA((24, SENDS)),
                pltpu.SemaphoreType.DMA((24, SENDS)),
            ],
            compiler_params=pltpu.CompilerParams(collective_id=0, has_side_effects=True, vmem_limit_bytes=limit),
            name="step",
        )(*g, *w, *state)
        near, moments = (pltpu.with_memory_space_constraint(x, pltpu.VMEM) for x in (near, moments))
        results = pl.pallas_call(
            store,
            out_shape=[jax.ShapeDtypeStruct((2, *whole), BF16)] * 3 + [jax.ShapeDtypeStruct((2, tiles, *tile), F32)] * 6,
            in_specs=[hbm, vmem, vmem],
            out_specs=[pl.BlockSpec(memory_space=pl.ANY)] * 9,
            scratch_shapes=[
                pltpu.VMEM((DEPTH, C, tiles, *tile), BF16),
                pltpu.SemaphoreType.DMA((DEPTH,)),
                pltpu.SemaphoreType.DMA((DEPTH,)),
                pltpu.SemaphoreType.DMA((12 - FAR,)),
            ],
            compiler_params=pltpu.CompilerParams(vmem_limit_bytes=limit),
            name="store",
        )(far, near, moments)
        return tuple(from_tiles(x, t.shape) for x, t in zip(results, (*weights, *m, *v), strict=True))

    all_of, cut = P(None, None, None), P(None, "dp", None)
    return jax.shard_map(
        step,
        mesh=mesh,
        in_specs=(P(("rep", "dp"), None, None, None),) * 3 + (all_of,) * 3 + (cut,) * 6,
        out_specs=(P("rep", None, None),) * 3 + (P("rep", "dp", None),) * 6,
        check_vma=False,
    )
```

```python
import functools

import jax
import jax.numpy as jnp
from jax import lax
from jax.experimental import pallas as pl
from jax.experimental.pallas import tpu as pltpu
from jax.sharding import PartitionSpec as P

MESH = pl.DeviceIdType.MESH
F32, BF16 = jnp.float32, jnp.bfloat16
Y, Z, C = 2, 4, 2
SPLIT = 16
RING = 8
SENDS = 4
DRAIN = 2
LAST = 10 + DRAIN
FAR = 3
DEPTH = 4
VMEM_BYTES = 67_043_328


def kernel(split, tiles, *refs):
    g, w, m, v = (refs[i : i + 3] for i in (0, 3, 6, 9))
    far, near, moments, ahead, own_a, part_a, own_b, part_b = refs[12:20]
    (y_a, l_a, r_a, sy_a, sl_a, sr_a, y_b, l_b, r_b, sy_b, sl_b, sr_b) = refs[20:32]
    (w_a, m_a, v_a, nw_a, w_b, m_b, v_b, nw_b) = refs[32:40]
    local_sem, send_sem, recv_sem, ahead_sem = refs[40:44]

    me = lax.axis_index("dp")
    c, z, y = lax.rem(me, C), lax.rem(lax.div(me, C), Z), lax.div(me, C * Z)
    other_c, other_y = 1 - c, 1 - y
    mate = {"dp": me + 1 - 2 * c}
    across = {"dp": me + (1 - 2 * y) * (Z * C)}
    right, left = {"dp": me + C}, {"dp": me - C}
    n = 6 * split
    big, small = 3 * tiles // 5 // split, 2 * tiles // 5 // split

    barrier = pltpu.get_barrier_semaphore()
    pl.semaphore_signal(barrier, inc=1, device_id=mate, device_id_type=MESH)
    pl.semaphore_signal(barrier, inc=1, device_id=across, device_id_type=MESH)

    @pl.when(z > 0)
    def _():
        pl.semaphore_signal(barrier, inc=1, device_id=left, device_id_type=MESH)

    @pl.when(z < Z - 1)
    def _():
        pl.semaphore_signal(barrier, inc=1, device_id=right, device_id_type=MESH)

    for ref in (l_a, l_b):
        ref[:, 0] = jnp.zeros_like(ref[:, 0])
    for ref in (r_a, r_b):
        ref[:, Z - 1] = jnp.zeros_like(ref[:, Z - 1])

    @pl.when((z > 0) & (z < Z - 1))
    def _():
        pl.semaphore_wait(barrier, 4)

    @pl.when((z == 0) | (z == Z - 1))
    def _():
        pl.semaphore_wait(barrier, 3)

    def remote(kind, q, src, dst, device):
        slot = lax.rem(q, SENDS)
        return pltpu.make_async_remote_copy(
            src_ref=src, dst_ref=dst, send_sem=send_sem.at[kind, slot], recv_sem=recv_sem.at[kind, slot], device_id=device, device_id_type=MESH
        )

    def local(kind, q, src, dst):
        return pltpu.make_async_copy(src, dst, local_sem.at[kind, lax.rem(q, SENDS)])

    def f(ref):
        return ref[...].astype(F32)

    def where(q):
        return lax.div(q, split), lax.rem(q, split)

    def by_weight(ml, act):
        for a in range(3):

            @pl.when(lax.div(ml, 2) == a)
            def _(a=a):
                act(a, lax.rem(ml, 2))

    def placed(q, act):
        ml = lax.div(q, split)

        @pl.when(ml < FAR)
        def _():
            act(far.at[ml])

        @pl.when(ml >= FAR)
        def _():
            act(near.at[ml - FAR])

    class Part:
        def __init__(self, which):
            self.which = which
            self.base = 12 * which
            self.count = (big, small)[which]
            self.first = (0, big * split)[which]
            self.own, self.part, self.ry, self.rl, self.rr, self.sy, self.sl, self.sr = (
                (own_a, part_a, y_a, l_a, r_a, sy_a, sl_a, sr_a),
                (own_b, part_b, y_b, l_b, r_b, sy_b, sl_b, sr_b),
            )[which]
            self.w, self.m, self.v, self.nw = ((w_a, m_a, v_a, nw_a), (w_b, m_b, v_b, nw_b))[which]

        def at(self, q):
            return pl.ds(self.first + lax.rem(q, split) * self.count, self.count)

        def remote(self, kind, q, src, dst, device):
            return remote(self.base + kind, q, src, dst, device)

        def local(self, kind, q, src, dst):
            return local(5 * self.which + kind, q, src, dst)

        def terms(self, q):
            slot = lax.rem(q, RING)

            def act(a, layer):
                self.remote(0, q, g[a].at[layer, :, :, other_c, self.at(q)], self.part.at[slot], mate).start()
                self.local(0, q, g[a].at[layer, :, :, c, self.at(q)], self.own.at[slot]).start()

            by_weight(where(q)[0], act)

        def terms_wait(self, q):
            slot = lax.rem(q, RING)
            self.local(0, q, self.own.at[slot], self.own.at[slot]).wait()
            self.remote(0, q, self.part.at[slot], self.part.at[slot], mate).wait_recv()

        def terms_sent(self, q):
            slot = lax.rem(q, RING)
            self.remote(0, q, self.part.at[slot], self.part.at[slot], mate).wait_send()

        def z_block(self, slot, j):
            raise NotImplementedError

        def z_send(self, q, h):
            slot, to = lax.rem(q, RING), lax.rem(q, SENDS)

            @pl.when(z == h - 1)
            def _():
                for j in range(h, Z):
                    self.z_sum(slot, j, self.sr.at[to, j], self.rl if h > 1 else None)
                self.remote(2, q, self.sr.at[to, h:Z], self.rl.at[slot, h:Z], right).start()

            @pl.when(z == Z - h)
            def _():
                for j in range(Z - h):
                    self.z_sum(slot, j, self.sl.at[to, j], self.rr if h > 1 else None)
                self.remote(3, q, self.sl.at[to, 0 : Z - h], self.rr.at[slot, 0 : Z - h], left).start()

        def z_wait(self, q, h):
            slot = lax.rem(q, RING)

            @pl.when(z == h)
            def _():
                self.remote(2, q, self.rl.at[slot, h:Z], self.rl.at[slot, h:Z], right).wait_recv()

            @pl.when(z == Z - 1 - h)
            def _():
                self.remote(3, q, self.rr.at[slot, 0 : Z - h], self.rr.at[slot, 0 : Z - h], left).wait_recv()

        def z_sent(self, q, h):
            to = lax.rem(q, SENDS)

            @pl.when(z == h - 1)
            def _():
                self.remote(2, q, self.sr.at[to, h:Z], self.sr.at[to, h:Z], right).wait_send()

            @pl.when(z == Z - h)
            def _():
                self.remote(3, q, self.sl.at[to, 0 : Z - h], self.sl.at[to, 0 : Z - h], left).wait_send()

        def state(self, q):
            slot = lax.rem(q, SENDS)

            def act(a, layer):
                self.local(1, q, w[a].at[layer, y, z, c, self.at(q)], self.w.at[slot]).start()
                self.local(2, q, m[a].at[layer, self.at(q)], self.m.at[slot]).start()
                self.local(3, q, v[a].at[layer, self.at(q)], self.v.at[slot]).start()

            by_weight(where(q)[0], act)

        def step(self, q, total):
            slot = lax.rem(q, SENDS)
            self.local(1, q, self.w.at[slot], self.w.at[slot]).wait()
            self.local(2, q, self.m.at[slot], self.m.at[slot]).wait()
            self.local(3, q, self.v.at[slot], self.v.at[slot]).wait()
            grad = total.astype(BF16).astype(F32)
            weight = f(self.w.at[slot])
            new_m = 0.9 * self.m[slot] + 0.1 * grad
            new_v = 0.95 * self.v[slot] + 0.05 * grad * grad
            ml, _ = where(q)
            moments[0, ml, self.at(q)] = new_m
            moments[1, ml, self.at(q)] = new_v
            new_w = (weight - 0.02 * (new_m * lax.rsqrt(new_v + 1e-8) + 0.1 * weight)).astype(BF16)
            self.nw[slot] = new_w

            @pl.when(ml < FAR)
            def _():
                self.local(4, q, self.nw.at[slot], far.at[ml, y, z, c, self.at(q)]).start()

            @pl.when(ml >= FAR)
            def _():
                near[ml - FAR, y, z, c, self.at(q)] = new_w

        def weight_stored(self, q):
            slot = lax.rem(q, SENDS)

            @pl.when(where(q)[0] < FAR)
            def _():
                self.local(4, q, self.nw.at[slot], self.nw.at[slot]).wait()

        def spread(self, q, h, src=None):
            def act(o):
                @pl.when((z >= h) & (z < Z - 1))
                def _():
                    dst = self.row(o, q, z - h)
                    self.remote(5 + h, q, dst if src is None else src, dst, right).start()

                @pl.when((z + h < Z) & (z > 0))
                def _():
                    dst = self.row(o, q, z + h)
                    self.remote(8 + h, q, dst if src is None else src, dst, left).start()

            placed(q, act)

        def spread_wait(self, q, h):
            def act(o):
                @pl.when(z > h)
                def _():
                    ref = self.row(o, q, z - h - 1)
                    self.remote(5 + h, q, ref, ref, right).wait_recv()

                @pl.when(z + h + 1 < Z)
                def _():
                    ref = self.row(o, q, z + h + 1)
                    self.remote(8 + h, q, ref, ref, left).wait_recv()

            placed(q, act)

        def spread_sent(self, q, h):
            def act(o):
                @pl.when((z >= h) & (z < Z - 1))
                def _():
                    ref = self.row(o, q, z - h)
                    self.remote(5 + h, q, ref, ref, right).wait_send()

                @pl.when((z + h < Z) & (z > 0))
                def _():
                    ref = self.row(o, q, z + h)
                    self.remote(8 + h, q, ref, ref, left).wait_send()

            placed(q, act)

        def share(self, q):
            def act(o):
                ref = o.at[:, :, c, self.at(q)]
                self.remote(11, q, ref, ref, mate).start()

            placed(q, act)

        def share_wait(self, q):
            def act(o):
                ref = o.at[:, :, other_c, self.at(q)]
                self.remote(11, q, ref, ref, mate).wait_recv()

            placed(q, act)

        def share_sent(self, q):
            def act(o):
                ref = o.at[:, :, c, self.at(q)]
                self.remote(11, q, ref, ref, mate).wait_send()

            placed(q, act)

    class YFirst(Part):
        def row(self, o, q, j):
            return o.at[y, j, c, self.at(q)]

        def z_sum(self, slot, j, to, more):
            total = f(self.own.at[slot, y, j]) + f(self.part.at[slot, y, j]) + f(self.ry.at[slot, j])
            to[...] = (total if more is None else total + f(more.at[slot, j])).astype(BF16)

        def y_send(self, q):
            slot, to = lax.rem(q, RING), lax.rem(q, SENDS)
            for j in range(Z):
                self.sy[to, j] = (f(self.own.at[slot, other_y, j]) + f(self.part.at[slot, other_y, j])).astype(BF16)
            self.remote(1, q, self.sy.at[to], self.ry.at[slot], across).start()

        def y_wait(self, q):
            slot = lax.rem(q, RING)
            self.remote(1, q, self.ry.at[slot], self.ry.at[slot], across).wait_recv()

        def y_sent(self, q):
            to = lax.rem(q, SENDS)
            self.remote(1, q, self.sy.at[to], self.sy.at[to], across).wait_send()

        def finish(self, q):
            slot = lax.rem(q, RING)
            total = f(self.own.at[slot, y, z]) + f(self.part.at[slot, y, z]) + f(self.ry.at[slot, z])
            self.step(q, total + f(self.rl.at[slot, z]) + f(self.rr.at[slot, z]))
            self.spread(q, 0, self.nw.at[lax.rem(q, SENDS)])

        def y_spread(self, q):
            def act(o):
                ref = o.at[y, :, c, self.at(q)]
                self.remote(4, q, ref, ref, across).start()

            placed(q, act)

        def y_spread_wait(self, q):
            def act(o):
                ref = o.at[other_y, :, c, self.at(q)]
                self.remote(4, q, ref, ref, across).wait_recv()

            placed(q, act)

        def y_spread_sent(self, q):
            def act(o):
                ref = o.at[y, :, c, self.at(q)]
                self.remote(4, q, ref, ref, across).wait_send()

            placed(q, act)

    class ZFirst(Part):
        def row(self, o, q, j):
            return o.at[:, j, c, self.at(q)]

        def z_sum(self, slot, j, to, more):
            for i in range(Y):
                total = f(self.own.at[slot, i, j]) + f(self.part.at[slot, i, j])
                to[i] = (total if more is None else total + f(more.at[slot, j, i])).astype(BF16)

        def column(self, slot, i):
            total = f(self.own.at[slot, i, z]) + f(self.part.at[slot, i, z])
            return total + f(self.rl.at[slot, z, i]) + f(self.rr.at[slot, z, i])

        def y_send(self, q):
            slot, to = lax.rem(q, RING), lax.rem(q, SENDS)
            self.sy[to] = self.column(slot, other_y).astype(BF16)
            self.remote(1, q, self.sy.at[to], self.ry.at[slot], across).start()

        def y_wait(self, q):
            slot = lax.rem(q, RING)
            self.remote(1, q, self.ry.at[slot], self.ry.at[slot], across).wait_recv()

        def y_sent(self, q):
            to = lax.rem(q, SENDS)
            self.remote(1, q, self.sy.at[to], self.sy.at[to], across).wait_send()

        def finish(self, q):
            slot = lax.rem(q, RING)
            self.step(q, self.column(slot, y) + f(self.ry.at[slot]))

            def act(o):
                self.remote(4, q, self.nw.at[lax.rem(q, SENDS)], o.at[y, z, c, self.at(q)], across).start()

            placed(q, act)

        def y_spread_wait(self, q):
            def act(o):
                ref = o.at[other_y, z, c, self.at(q)]
                self.remote(4, q, ref, ref, across).wait_recv()

            placed(q, act)

        def y_spread_sent(self, q):
            def act(o):
                ref = o.at[y, z, c, self.at(q)]
                self.remote(4, q, ref, ref, across).wait_send()

            placed(q, act)

    a, b = YFirst(0), ZFirst(1)

    def early():
        source = far.at[FAR - 1]
        pairs = held_pieces(split, tiles, source, (ahead, own_a, part_a, own_b, part_b))
        return [pltpu.make_async_copy(src, dst, ahead_sem.at[i]) for i, (src, dst) in enumerate(pairs)]

    def iteration(t, _):
        def at(stage, *acts):
            q = t - stage

            @pl.when((q >= 0) & (q < n))
            def _():
                for act in acts:
                    act(q)

        def hop(act, h):
            return lambda q: act(q, h)

        at(0, a.terms, b.terms)
        at(0 + DRAIN, a.terms_sent, b.terms_sent)
        at(1 + DRAIN, a.y_sent, hop(b.z_sent, 1))
        at(2 + DRAIN, hop(a.z_sent, 1), hop(b.z_sent, 2))
        at(3 + DRAIN, hop(a.z_sent, 2), hop(b.z_sent, 3))
        at(4 + DRAIN, hop(a.z_sent, 3), b.y_sent)
        at(5 + DRAIN, hop(a.spread_sent, 0), b.y_spread_sent)
        at(6 + DRAIN, hop(a.spread_sent, 1), hop(b.spread_sent, 0))
        at(7 + DRAIN, hop(a.spread_sent, 2), hop(b.spread_sent, 1))
        at(8 + DRAIN, a.y_spread_sent, hop(b.spread_sent, 2))
        at(9 + DRAIN, a.share_sent, b.share_sent)
        at(3, a.state, b.state)
        at(1, a.terms_wait, a.y_send)
        at(8, hop(a.spread_wait, 2), a.y_spread)
        at(7, hop(a.spread_wait, 1), hop(a.spread, 2))
        at(6, a.weight_stored, hop(a.spread_wait, 0), hop(a.spread, 1))
        at(2, a.y_wait, hop(a.z_send, 1))
        at(3, hop(a.z_wait, 1), hop(a.z_send, 2))
        at(4, hop(a.z_wait, 2), hop(a.z_send, 3))
        at(5, hop(a.z_wait, 3), a.finish)
        at(9, a.y_spread_wait, a.share)
        at(1, b.terms_wait, hop(b.z_send, 1))
        at(8, hop(b.spread_wait, 1), hop(b.spread, 2))
        at(7, hop(b.spread_wait, 0), hop(b.spread, 1))
        at(6, b.weight_stored, b.y_spread_wait, hop(b.spread, 0))
        at(2, hop(b.z_wait, 1), hop(b.z_send, 2))
        at(3, hop(b.z_wait, 2), hop(b.z_send, 3))
        at(4, hop(b.z_wait, 3), b.y_send)
        at(5, b.y_wait, b.finish)
        at(9, hop(b.spread_wait, 2), b.share)
        at(10, a.share_wait, b.share_wait)

        @pl.when(t == n + 5)
        def _():
            for copy in early():
                copy.start()

        return 0

    lax.fori_loop(0, n + LAST, iteration, 0)
    for copy in early():
        copy.wait()


def held_pieces(split, tiles, whole, held):
    ahead, *slots = held
    pairs = [(whole.at[:, :, 1], ahead)]
    first = 0
    for own, part in (slots[:2], slots[2:]):
        count = own.shape[3]
        for r in range(split):
            piece = whole.at[:, :, 0, first + r * count : first + (r + 1) * count]
            pairs.append((piece, (own if r < RING else part).at[r % RING]))
        first += count * split
    return pairs


def store(split, tiles, far, near, moments, *refs):
    early, new, states, (line, read_sem, write_sem, held_sem) = refs[:5], refs[5:8], refs[8:14], refs[14:]
    pieces = [(ml, j) for ml in range(FAR - 1) for j in range(Y * Z)]

    def read(i):
        ml, j = pieces[i]
        return pltpu.make_async_copy(far.at[ml, j // Z, j % Z], line.at[i % DEPTH], read_sem.at[i % DEPTH])

    def write(i):
        ml, j = pieces[i]
        return pltpu.make_async_copy(line.at[i % DEPTH], new[ml // 2].at[ml % 2, j // Z, j % Z], write_sem.at[i % DEPTH])

    held = [(near.at[ml - FAR], new[ml // 2].at[ml % 2]) for ml in range(FAR, 6)]
    held += [(moments.at[i // 3, 2 * (i % 3) : 2 * (i % 3) + 2], states[i]) for i in range(6)]
    held += [(src, dst) for dst, src in held_pieces(split, tiles, new[(FAR - 1) // 2].at[(FAR - 1) % 2], early)]
    held = [pltpu.make_async_copy(src, dst, held_sem.at[i]) for i, (src, dst) in enumerate(held)]
    for i in range(DEPTH):
        read(i).start()
    for copy in held:
        copy.start()
    for i in range(len(pieces)):
        read(i).wait()
        write(i).start()
        if i >= 1 and i - 1 + DEPTH < len(pieces):
            write(i - 1).wait()
            read(i - 1 + DEPTH).start()
    for i in range(len(pieces) - DEPTH, len(pieces)):
        write(i).wait()
    for copy in held:
        copy.wait()


def to_tiles(x, lead):
    *head, rows, columns = x.shape
    k = len(head)
    x = x.reshape(*head, rows // 8, 8, columns // 128, 128).transpose(*range(k), k, k + 2, k + 1, k + 3)
    return x.reshape(*lead, -1, 8, 128)


def from_tiles(x, shape):
    *head, rows, columns = shape
    k = len(head)
    x = x.reshape(*head, rows // 8, columns // 128, 8, 128).transpose(*range(k), k, k + 2, k + 1, k + 3)
    return x.reshape(shape)


def solution(mesh, split=SPLIT):
    def step(*arrays):
        terms, weights, m, v = (arrays[i : i + 3] for i in (0, 3, 6, 9))
        g = [to_tiles(t[0], (2, Y, Z, C)) for t in terms]
        w = [to_tiles(t, (2, Y, Z, C)) for t in weights]
        state = [to_tiles(t, (2,)) for t in (*m, *v)]
        tiles = state[0].shape[1]
        tile = (8, 128)
        limit = VMEM_BYTES - 1024 * tiles * (2 * Y * Z * C * (6 - FAR) + 4 * 2 * 6 + 2 * Y * Z)
        limit -= 2 * 1024 * 2 * RING * Y * Z * tiles // split

        def buffers(count, line):
            one = (count, *tile)
            blocks = [(RING, *((Z,) if line == () else ()), *one)] + [(RING, Z, *line, *one)] * 2
            sent = [(SENDS, *((Z,) if line == () else ()), *one)] + [(SENDS, Z, *line, *one)] * 2
            return [pltpu.VMEM(shape, BF16) for shape in blocks + sent]

        big, small = 3 * tiles // 5 // split, 2 * tiles // 5 // split
        held = [pltpu.VMEM((SENDS, count, *tile), t) for count in (big, small) for t in (BF16, F32, F32, BF16)]
        whole = (Y, Z, C, tiles, *tile)
        hbm, vmem = pl.BlockSpec(memory_space=pltpu.HBM), pl.BlockSpec(memory_space=pltpu.VMEM)
        terms_of = [(RING, Y, Z, count, *tile) for count in (big, big, small, small)]
        far, *kept = pl.pallas_call(
            functools.partial(kernel, split, tiles),
            out_shape=(
                pltpu.HBM((FAR, *whole), BF16),
                pltpu.VMEM((6 - FAR, *whole), BF16),
                pltpu.VMEM((2, 6, tiles, *tile), F32),
                pltpu.VMEM((Y, Z, tiles, *tile), BF16),
                *(pltpu.VMEM(shape, BF16) for shape in terms_of),
            ),
            in_specs=[pl.BlockSpec(memory_space=pl.ANY)] * 12,
            out_specs=(hbm,) + (vmem,) * 7,
            scratch_shapes=[
                *buffers(big, ()),
                *buffers(small, (Y,)),
                *held,
                pltpu.SemaphoreType.DMA((10, SENDS)),
                pltpu.SemaphoreType.DMA((24, SENDS)),
                pltpu.SemaphoreType.DMA((24, SENDS)),
                pltpu.SemaphoreType.DMA((1 + 2 * split,)),
            ],
            compiler_params=pltpu.CompilerParams(collective_id=0, has_side_effects=True, vmem_limit_bytes=limit),
            name="step",
        )(*g, *w, *state)
        kept = [pltpu.with_memory_space_constraint(x, pltpu.VMEM) for x in kept]
        results = pl.pallas_call(
            functools.partial(store, split, tiles),
            out_shape=[jax.ShapeDtypeStruct((2, *whole), BF16)] * 3 + [jax.ShapeDtypeStruct((2, tiles, *tile), F32)] * 6,
            in_specs=[hbm] + [vmem] * 7,
            out_specs=[pl.BlockSpec(memory_space=pl.ANY)] * 9,
            scratch_shapes=[
                pltpu.VMEM((DEPTH, C, tiles, *tile), BF16),
                pltpu.SemaphoreType.DMA((DEPTH,)),
                pltpu.SemaphoreType.DMA((DEPTH,)),
                pltpu.SemaphoreType.DMA((13 - FAR + 2 * split,)),
            ],
            compiler_params=pltpu.CompilerParams(vmem_limit_bytes=limit),
            name="store",
        )(far, *kept)
        return tuple(from_tiles(x, t.shape) for x, t in zip(results, (*weights, *m, *v), strict=True))

    all_of, cut = P(None, None, None), P(None, "dp", None)
    return jax.shard_map(
        step,
        mesh=mesh,
        in_specs=(P(("rep", "dp"), None, None, None),) * 3 + (all_of,) * 3 + (cut,) * 6,
        out_specs=(P("rep", None, None),) * 3 + (P("rep", "dp", None),) * 6,
        check_vma=False,
    )
```

```python
import functools

import jax
import jax.numpy as jnp
from jax import lax
from jax.experimental import pallas as pl
from jax.experimental.pallas import tpu as pltpu
from jax.sharding import PartitionSpec as P

MESH = pl.DeviceIdType.MESH
F32, BF16 = jnp.float32, jnp.bfloat16
Y, Z, C = 2, 4, 2
SPLIT = 16
RING = 8
SENDS = 4
SEMS = 8
DRAIN = 2
SHORT = 2
LAST = 9
FAR = 3
DEPTH = 4
VMEM_BYTES = 67_043_328


def kernel(split, tiles, *refs):
    g, w, m, v = (refs[i : i + 3] for i in (0, 3, 6, 9))
    far, near, moments, ahead, own_a, part_a, own_b, part_b = refs[12:20]
    (y_a, l_a, r_a, sy_a, sl_a, sr_a, y_b, l_b, r_b, sy_b, sl_b, sr_b) = refs[20:32]
    (w_a, m_a, v_a, nw_a, w_b, m_b, v_b, nw_b) = refs[32:40]
    local_sem, send_sem, recv_sem, ahead_sem = refs[40:44]

    me = lax.axis_index("dp")
    c, z, y = lax.rem(me, C), lax.rem(lax.div(me, C), Z), lax.div(me, C * Z)
    other_c, other_y = 1 - c, 1 - y
    mate = {"dp": me + 1 - 2 * c}
    across = {"dp": me + (1 - 2 * y) * (Z * C)}
    right, left = {"dp": me + C}, {"dp": me - C}
    n = 6 * split
    big, small = 3 * tiles // 5 // split, 2 * tiles // 5 // split

    barrier = pltpu.get_barrier_semaphore()
    pl.semaphore_signal(barrier, inc=1, device_id=mate, device_id_type=MESH)
    pl.semaphore_signal(barrier, inc=1, device_id=across, device_id_type=MESH)

    @pl.when(z > 0)
    def _():
        pl.semaphore_signal(barrier, inc=1, device_id=left, device_id_type=MESH)

    @pl.when(z < Z - 1)
    def _():
        pl.semaphore_signal(barrier, inc=1, device_id=right, device_id_type=MESH)

    for ref in (l_a, l_b):
        ref[:, 0] = jnp.zeros_like(ref[:, 0])
    for ref in (r_a, r_b):
        ref[:, Z - 1] = jnp.zeros_like(ref[:, Z - 1])

    @pl.when((z > 0) & (z < Z - 1))
    def _():
        pl.semaphore_wait(barrier, 4)

    @pl.when((z == 0) | (z == Z - 1))
    def _():
        pl.semaphore_wait(barrier, 3)

    def remote(kind, q, src, dst, device):
        slot = lax.rem(q, SEMS)
        return pltpu.make_async_remote_copy(
            src_ref=src, dst_ref=dst, send_sem=send_sem.at[kind, slot], recv_sem=recv_sem.at[kind, slot], device_id=device, device_id_type=MESH
        )

    def local(kind, q, src, dst):
        return pltpu.make_async_copy(src, dst, local_sem.at[kind, lax.rem(q, SENDS)])

    def f(ref):
        return ref[...].astype(F32)

    def where(q):
        return lax.div(q, split), lax.rem(q, split)

    def by_weight(ml, act):
        for a in range(3):

            @pl.when(lax.div(ml, 2) == a)
            def _(a=a):
                act(a, lax.rem(ml, 2))

    def placed(q, act):
        ml = lax.div(q, split)

        @pl.when(ml < FAR)
        def _():
            act(far.at[ml])

        @pl.when(ml >= FAR)
        def _():
            act(near.at[ml - FAR])

    class Part:
        def __init__(self, which):
            self.which = which
            self.base = 12 * which
            self.count = (big, small)[which]
            self.first = (0, big * split)[which]
            self.own, self.part, self.ry, self.rl, self.rr, self.sy, self.sl, self.sr = (
                (own_a, part_a, y_a, l_a, r_a, sy_a, sl_a, sr_a),
                (own_b, part_b, y_b, l_b, r_b, sy_b, sl_b, sr_b),
            )[which]
            self.w, self.m, self.v, self.nw = ((w_a, m_a, v_a, nw_a), (w_b, m_b, v_b, nw_b))[which]

        def at(self, q):
            return pl.ds(self.first + lax.rem(q, split) * self.count, self.count)

        def remote(self, kind, q, src, dst, device):
            return remote(self.base + kind, q, src, dst, device)

        def local(self, kind, q, src, dst):
            return local(5 * self.which + kind, q, src, dst)

        def terms(self, q):
            slot = lax.rem(q, RING)

            def act(a, layer):
                self.remote(0, q, g[a].at[layer, :, :, other_c, self.at(q)], self.part.at[slot], mate).start()
                self.local(0, q, g[a].at[layer, :, :, c, self.at(q)], self.own.at[slot]).start()

            by_weight(where(q)[0], act)

        def terms_wait(self, q):
            slot = lax.rem(q, RING)
            self.local(0, q, self.own.at[slot], self.own.at[slot]).wait()
            self.remote(0, q, self.part.at[slot], self.part.at[slot], mate).wait_recv()

        def terms_sent(self, q):
            slot = lax.rem(q, RING)
            self.remote(0, q, self.part.at[slot], self.part.at[slot], mate).wait_send()

        def z_block(self, slot, j):
            raise NotImplementedError

        def z_send(self, q, h):
            slot, to = lax.rem(q, RING), lax.rem(q, SENDS)

            @pl.when(z == h - 1)
            def _():
                for j in range(h, Z):
                    self.z_sum(slot, j, self.sr.at[to, j], self.rl if h > 1 else None)
                self.remote(2, q, self.sr.at[to, h:Z], self.rl.at[slot, h:Z], right).start()

            @pl.when(z == Z - h)
            def _():
                for j in range(Z - h):
                    self.z_sum(slot, j, self.sl.at[to, j], self.rr if h > 1 else None)
                self.remote(3, q, self.sl.at[to, 0 : Z - h], self.rr.at[slot, 0 : Z - h], left).start()

        def z_wait(self, q, h):
            slot = lax.rem(q, RING)

            @pl.when(z == h)
            def _():
                self.remote(2, q, self.rl.at[slot, h:Z], self.rl.at[slot, h:Z], right).wait_recv()

            @pl.when(z == Z - 1 - h)
            def _():
                self.remote(3, q, self.rr.at[slot, 0 : Z - h], self.rr.at[slot, 0 : Z - h], left).wait_recv()

        def z_sent(self, q, h):
            to = lax.rem(q, SENDS)

            @pl.when(z == h - 1)
            def _():
                self.remote(2, q, self.sr.at[to, h:Z], self.sr.at[to, h:Z], right).wait_send()

            @pl.when(z == Z - h)
            def _():
                self.remote(3, q, self.sl.at[to, 0 : Z - h], self.sl.at[to, 0 : Z - h], left).wait_send()

        def state(self, q):
            slot = lax.rem(q, SENDS)

            def act(a, layer):
                self.local(1, q, w[a].at[layer, y, z, c, self.at(q)], self.w.at[slot]).start()
                self.local(2, q, m[a].at[layer, self.at(q)], self.m.at[slot]).start()
                self.local(3, q, v[a].at[layer, self.at(q)], self.v.at[slot]).start()

            by_weight(where(q)[0], act)

        def step(self, q, total):
            slot = lax.rem(q, SENDS)
            self.local(1, q, self.w.at[slot], self.w.at[slot]).wait()
            self.local(2, q, self.m.at[slot], self.m.at[slot]).wait()
            self.local(3, q, self.v.at[slot], self.v.at[slot]).wait()
            grad = total.astype(BF16).astype(F32)
            weight = f(self.w.at[slot])
            new_m = 0.9 * self.m[slot] + 0.1 * grad
            new_v = 0.95 * self.v[slot] + 0.05 * grad * grad
            ml, _ = where(q)
            moments[0, ml, self.at(q)] = new_m
            moments[1, ml, self.at(q)] = new_v
            new_w = (weight - 0.02 * (new_m * lax.rsqrt(new_v + 1e-8) + 0.1 * weight)).astype(BF16)
            self.nw[slot] = new_w

            @pl.when(ml < FAR)
            def _():
                self.local(4, q, self.nw.at[slot], far.at[ml, y, z, c, self.at(q)]).start()

            @pl.when(ml >= FAR)
            def _():
                near[ml - FAR, y, z, c, self.at(q)] = new_w

        def weight_stored(self, q):
            slot = lax.rem(q, SENDS)

            @pl.when(where(q)[0] < FAR)
            def _():
                self.local(4, q, self.nw.at[slot], self.nw.at[slot]).wait()

        def spread(self, q, h, src=None):
            def act(o):
                @pl.when((z >= h) & (z < Z - 1))
                def _():
                    dst = self.row(o, q, z - h)
                    self.remote(5 + h, q, dst if src is None else src, dst, right).start()

                @pl.when((z + h < Z) & (z > 0))
                def _():
                    dst = self.row(o, q, z + h)
                    self.remote(8 + h, q, dst if src is None else src, dst, left).start()

            placed(q, act)

        def spread_wait(self, q, h):
            def act(o):
                @pl.when(z > h)
                def _():
                    ref = self.row(o, q, z - h - 1)
                    self.remote(5 + h, q, ref, ref, right).wait_recv()

                @pl.when(z + h + 1 < Z)
                def _():
                    ref = self.row(o, q, z + h + 1)
                    self.remote(8 + h, q, ref, ref, left).wait_recv()

            placed(q, act)

        def spread_sent(self, q, h):
            def act(o):
                @pl.when((z >= h) & (z < Z - 1))
                def _():
                    ref = self.row(o, q, z - h)
                    self.remote(5 + h, q, ref, ref, right).wait_send()

                @pl.when((z + h < Z) & (z > 0))
                def _():
                    ref = self.row(o, q, z + h)
                    self.remote(8 + h, q, ref, ref, left).wait_send()

            placed(q, act)

        def straight(self, q, src=None):
            def act(o):
                ref = self.row(o, q, z)
                for h in range(Z - 1):

                    @pl.when(z + h + 1 < Z)
                    def _(h=h):
                        self.remote(5 + h, q, ref if src is None else src, ref, {"dp": me + (h + 1) * C}).start()

                    @pl.when(z > h)
                    def _(h=h):
                        self.remote(8 + h, q, ref if src is None else src, ref, {"dp": me - (h + 1) * C}).start()

            placed(q, act)

        def straight_wait(self, q):
            for h in range(Z - 1):
                self.spread_wait(q, h)

        def straight_sent(self, q):
            def act(o):
                ref = self.row(o, q, z)
                for h in range(Z - 1):

                    @pl.when(z + h + 1 < Z)
                    def _(h=h):
                        self.remote(5 + h, q, ref, ref, {"dp": me + (h + 1) * C}).wait_send()

                    @pl.when(z > h)
                    def _(h=h):
                        self.remote(8 + h, q, ref, ref, {"dp": me - (h + 1) * C}).wait_send()

            placed(q, act)

        def share(self, q):
            def act(o):
                ref = o.at[:, :, c, self.at(q)]
                self.remote(11, q, ref, ref, mate).start()

            placed(q, act)

        def share_wait(self, q):
            def act(o):
                ref = o.at[:, :, other_c, self.at(q)]
                self.remote(11, q, ref, ref, mate).wait_recv()

            placed(q, act)

        def share_sent(self, q):
            def act(o):
                ref = o.at[:, :, c, self.at(q)]
                self.remote(11, q, ref, ref, mate).wait_send()

            placed(q, act)

    class YFirst(Part):
        def row(self, o, q, j):
            return o.at[y, j, c, self.at(q)]

        def z_sum(self, slot, j, to, more):
            total = f(self.own.at[slot, y, j]) + f(self.part.at[slot, y, j]) + f(self.ry.at[slot, j])
            to[...] = (total if more is None else total + f(more.at[slot, j])).astype(BF16)

        def y_send(self, q):
            slot, to = lax.rem(q, RING), lax.rem(q, SENDS)
            for j in range(Z):
                self.sy[to, j] = (f(self.own.at[slot, other_y, j]) + f(self.part.at[slot, other_y, j])).astype(BF16)
            self.remote(1, q, self.sy.at[to], self.ry.at[slot], across).start()

        def y_wait(self, q):
            slot = lax.rem(q, RING)
            self.remote(1, q, self.ry.at[slot], self.ry.at[slot], across).wait_recv()

        def y_sent(self, q):
            to = lax.rem(q, SENDS)
            self.remote(1, q, self.sy.at[to], self.sy.at[to], across).wait_send()

        def finish(self, q):
            slot = lax.rem(q, RING)
            total = f(self.own.at[slot, y, z]) + f(self.part.at[slot, y, z]) + f(self.ry.at[slot, z])
            self.step(q, total + f(self.rl.at[slot, z]) + f(self.rr.at[slot, z]))

            @pl.when(q < n - SHORT)
            def _():
                self.spread(q, 0, self.nw.at[lax.rem(q, SENDS)])

            @pl.when(q >= n - SHORT)
            def _():
                self.straight(q, self.nw.at[lax.rem(q, SENDS)])

        def y_spread(self, q):
            def act(o):
                ref = o.at[y, :, c, self.at(q)]
                self.remote(4, q, ref, ref, across).start()

            placed(q, act)

        def y_spread_wait(self, q):
            def act(o):
                ref = o.at[other_y, :, c, self.at(q)]
                self.remote(4, q, ref, ref, across).wait_recv()

            placed(q, act)

        def y_spread_sent(self, q):
            def act(o):
                ref = o.at[y, :, c, self.at(q)]
                self.remote(4, q, ref, ref, across).wait_send()

            placed(q, act)

    class ZFirst(Part):
        def row(self, o, q, j):
            return o.at[:, j, c, self.at(q)]

        def z_sum(self, slot, j, to, more):
            for i in range(Y):
                total = f(self.own.at[slot, i, j]) + f(self.part.at[slot, i, j])
                to[i] = (total if more is None else total + f(more.at[slot, j, i])).astype(BF16)

        def column(self, slot, i):
            total = f(self.own.at[slot, i, z]) + f(self.part.at[slot, i, z])
            return total + f(self.rl.at[slot, z, i]) + f(self.rr.at[slot, z, i])

        def y_send(self, q):
            slot, to = lax.rem(q, RING), lax.rem(q, SENDS)
            self.sy[to] = self.column(slot, other_y).astype(BF16)
            self.remote(1, q, self.sy.at[to], self.ry.at[slot], across).start()

        def y_wait(self, q):
            slot = lax.rem(q, RING)
            self.remote(1, q, self.ry.at[slot], self.ry.at[slot], across).wait_recv()

        def y_sent(self, q):
            to = lax.rem(q, SENDS)
            self.remote(1, q, self.sy.at[to], self.sy.at[to], across).wait_send()

        def finish(self, q):
            slot = lax.rem(q, RING)
            self.step(q, self.column(slot, y) + f(self.ry.at[slot]))

            def act(o):
                self.remote(4, q, self.nw.at[lax.rem(q, SENDS)], o.at[y, z, c, self.at(q)], across).start()

            placed(q, act)

        def y_spread_wait(self, q):
            def act(o):
                ref = o.at[other_y, z, c, self.at(q)]
                self.remote(4, q, ref, ref, across).wait_recv()

            placed(q, act)

        def y_spread_sent(self, q):
            def act(o):
                ref = o.at[y, z, c, self.at(q)]
                self.remote(4, q, ref, ref, across).wait_send()

            placed(q, act)

    a, b = YFirst(0), ZFirst(1)

    def early():
        source = far.at[FAR - 1]
        pairs = held_pieces(split, tiles, source, (ahead, own_a, part_a, own_b, part_b))
        return [pltpu.make_async_copy(src, dst, ahead_sem.at[i]) for i, (src, dst) in enumerate(pairs)]

    def iteration(t, _):
        def at(stage, *acts, first=0, end=n):
            q = t - stage

            @pl.when((q >= first) & (q < end))
            def _():
                for act in acts:
                    act(q)

        long, short = {"end": n - SHORT}, {"first": n - SHORT}

        def hop(act, h):
            return lambda q: act(q, h)

        at(0, a.terms, b.terms)
        at(0 + DRAIN, a.terms_sent, b.terms_sent)
        at(1 + DRAIN, a.y_sent, hop(b.z_sent, 1))
        at(2 + DRAIN, hop(a.z_sent, 1), hop(b.z_sent, 2))
        at(3 + DRAIN, hop(a.z_sent, 2), hop(b.z_sent, 3))
        at(4 + DRAIN, hop(a.z_sent, 3), b.y_sent)
        at(5 + DRAIN, b.y_spread_sent)
        at(5 + DRAIN, hop(a.spread_sent, 0), **long)
        at(6 + DRAIN, hop(a.spread_sent, 1), hop(b.spread_sent, 0), **long)
        at(7 + DRAIN, hop(a.spread_sent, 2), hop(b.spread_sent, 1), **long)
        at(8 + DRAIN, a.y_spread_sent, hop(b.spread_sent, 2), **long)
        at(9 + DRAIN, a.share_sent, b.share_sent, **long)
        at(3, a.state, b.state)
        at(1, a.terms_wait, a.y_send)
        at(8, hop(a.spread_wait, 2), a.y_spread, **long)
        at(7, hop(a.spread_wait, 1), hop(a.spread, 2), **long)
        at(6, a.weight_stored, hop(a.spread_wait, 0), hop(a.spread, 1), **long)
        at(6, a.weight_stored, a.straight_wait, a.y_spread, **short)
        at(2, a.y_wait, hop(a.z_send, 1))
        at(3, hop(a.z_wait, 1), hop(a.z_send, 2))
        at(4, hop(a.z_wait, 2), hop(a.z_send, 3))
        at(5, hop(a.z_wait, 3), a.finish)
        at(9, a.y_spread_wait, a.share, **long)
        at(7, a.y_spread_wait, a.share, **short)
        at(1, b.terms_wait, hop(b.z_send, 1))
        at(8, hop(b.spread_wait, 1), hop(b.spread, 2), **long)
        at(7, hop(b.spread_wait, 0), hop(b.spread, 1), **long)
        at(6, b.weight_stored, b.y_spread_wait, hop(b.spread, 0), **long)
        at(6, b.weight_stored, b.y_spread_wait, b.straight, **short)
        at(2, hop(b.z_wait, 1), hop(b.z_send, 2))
        at(3, hop(b.z_wait, 2), hop(b.z_send, 3))
        at(4, hop(b.z_wait, 3), b.y_send)
        at(5, b.y_wait, b.finish)
        at(9, hop(b.spread_wait, 2), b.share, **long)
        at(7, b.straight_wait, b.share, **short)
        at(10, a.share_wait, b.share_wait, **long)
        at(8, a.share_wait, b.share_wait, **short)
        at(9, a.straight_sent, b.straight_sent, a.y_spread_sent, a.share_sent, b.share_sent, **short)

        @pl.when(t == n + 5)
        def _():
            for copy in early():
                copy.start()

        return 0

    lax.fori_loop(0, n + LAST, iteration, 0)
    for copy in early():
        copy.wait()


def held_pieces(split, tiles, whole, held):
    ahead, *slots = held
    pairs = [(whole.at[:, :, 1], ahead)]
    first = 0
    for own, part in (slots[:2], slots[2:]):
        count = own.shape[3]
        for r in range(split):
            piece = whole.at[:, :, 0, first + r * count : first + (r + 1) * count]
            pairs.append((piece, (own if r < RING else part).at[r % RING]))
        first += count * split
    return pairs


def store(split, tiles, far, near, moments, *refs):
    early, new, states, (line, read_sem, write_sem, held_sem) = refs[:5], refs[5:8], refs[8:14], refs[14:]
    pieces = [(ml, j) for ml in range(FAR - 1) for j in range(Y * Z)]

    def read(i):
        ml, j = pieces[i]
        return pltpu.make_async_copy(far.at[ml, j // Z, j % Z], line.at[i % DEPTH], read_sem.at[i % DEPTH])

    def write(i):
        ml, j = pieces[i]
        return pltpu.make_async_copy(line.at[i % DEPTH], new[ml // 2].at[ml % 2, j // Z, j % Z], write_sem.at[i % DEPTH])

    held = [(near.at[ml - FAR], new[ml // 2].at[ml % 2]) for ml in range(FAR, 6)]
    held += [(moments.at[i // 3, 2 * (i % 3) : 2 * (i % 3) + 2], states[i]) for i in range(6)]
    held += [(src, dst) for dst, src in held_pieces(split, tiles, new[(FAR - 1) // 2].at[(FAR - 1) % 2], early)]
    held = [pltpu.make_async_copy(src, dst, held_sem.at[i]) for i, (src, dst) in enumerate(held)]
    for i in range(DEPTH):
        read(i).start()
    for copy in held:
        copy.start()
    for i in range(len(pieces)):
        read(i).wait()
        write(i).start()
        if i >= 1 and i - 1 + DEPTH < len(pieces):
            write(i - 1).wait()
            read(i - 1 + DEPTH).start()
    for i in range(len(pieces) - DEPTH, len(pieces)):
        write(i).wait()
    for copy in held:
        copy.wait()


def to_tiles(x, lead):
    *head, rows, columns = x.shape
    k = len(head)
    x = x.reshape(*head, rows // 8, 8, columns // 128, 128).transpose(*range(k), k, k + 2, k + 1, k + 3)
    return x.reshape(*lead, -1, 8, 128)


def from_tiles(x, shape):
    *head, rows, columns = shape
    k = len(head)
    x = x.reshape(*head, rows // 8, columns // 128, 8, 128).transpose(*range(k), k, k + 2, k + 1, k + 3)
    return x.reshape(shape)


def solution(mesh, split=SPLIT):
    def step(*arrays):
        terms, weights, m, v = (arrays[i : i + 3] for i in (0, 3, 6, 9))
        g = [to_tiles(t[0], (2, Y, Z, C)) for t in terms]
        w = [to_tiles(t, (2, Y, Z, C)) for t in weights]
        state = [to_tiles(t, (2,)) for t in (*m, *v)]
        tiles = state[0].shape[1]
        tile = (8, 128)
        limit = VMEM_BYTES - 1024 * tiles * (2 * Y * Z * C * (6 - FAR) + 4 * 2 * 6 + 2 * Y * Z)
        limit -= 2 * 1024 * 2 * RING * Y * Z * tiles // split

        def buffers(count, line):
            one = (count, *tile)
            blocks = [(RING, *((Z,) if line == () else ()), *one)] + [(RING, Z, *line, *one)] * 2
            sent = [(SENDS, *((Z,) if line == () else ()), *one)] + [(SENDS, Z, *line, *one)] * 2
            return [pltpu.VMEM(shape, BF16) for shape in blocks + sent]

        big, small = 3 * tiles // 5 // split, 2 * tiles // 5 // split
        held = [pltpu.VMEM((SENDS, count, *tile), t) for count in (big, small) for t in (BF16, F32, F32, BF16)]
        whole = (Y, Z, C, tiles, *tile)
        hbm, vmem = pl.BlockSpec(memory_space=pltpu.HBM), pl.BlockSpec(memory_space=pltpu.VMEM)
        terms_of = [(RING, Y, Z, count, *tile) for count in (big, big, small, small)]
        far, *kept = pl.pallas_call(
            functools.partial(kernel, split, tiles),
            out_shape=(
                pltpu.HBM((FAR, *whole), BF16),
                pltpu.VMEM((6 - FAR, *whole), BF16),
                pltpu.VMEM((2, 6, tiles, *tile), F32),
                pltpu.VMEM((Y, Z, tiles, *tile), BF16),
                *(pltpu.VMEM(shape, BF16) for shape in terms_of),
            ),
            in_specs=[pl.BlockSpec(memory_space=pl.ANY)] * 12,
            out_specs=(hbm,) + (vmem,) * 7,
            scratch_shapes=[
                *buffers(big, ()),
                *buffers(small, (Y,)),
                *held,
                pltpu.SemaphoreType.DMA((10, SENDS)),
                pltpu.SemaphoreType.DMA((24, SEMS)),
                pltpu.SemaphoreType.DMA((24, SEMS)),
                pltpu.SemaphoreType.DMA((1 + 2 * split,)),
            ],
            compiler_params=pltpu.CompilerParams(collective_id=0, has_side_effects=True, vmem_limit_bytes=limit),
            name="step",
        )(*g, *w, *state)
        kept = [pltpu.with_memory_space_constraint(x, pltpu.VMEM) for x in kept]
        results = pl.pallas_call(
            functools.partial(store, split, tiles),
            out_shape=[jax.ShapeDtypeStruct((2, *whole), BF16)] * 3 + [jax.ShapeDtypeStruct((2, tiles, *tile), F32)] * 6,
            in_specs=[hbm] + [vmem] * 7,
            out_specs=[pl.BlockSpec(memory_space=pl.ANY)] * 9,
            scratch_shapes=[
                pltpu.VMEM((DEPTH, C, tiles, *tile), BF16),
                pltpu.SemaphoreType.DMA((DEPTH,)),
                pltpu.SemaphoreType.DMA((DEPTH,)),
                pltpu.SemaphoreType.DMA((13 - FAR + 2 * split,)),
            ],
            compiler_params=pltpu.CompilerParams(vmem_limit_bytes=limit),
            name="store",
        )(far, *kept)
        return tuple(from_tiles(x, t.shape) for x, t in zip(results, (*weights, *m, *v), strict=True))

    all_of, cut = P(None, None, None), P(None, "dp", None)
    return jax.shard_map(
        step,
        mesh=mesh,
        in_specs=(P(("rep", "dp"), None, None, None),) * 3 + (all_of,) * 3 + (cut,) * 6,
        out_specs=(P("rep", None, None),) * 3 + (P("rep", "dp", None),) * 6,
        check_vma=False,
    )
```
